32 devices in a mesh: grp: 4 (over z), dev: 8 (over y, x, core).
Axes of the slice: x: 2, y: 2, z: 4, core: 2. Of those that a mesh axis runs over, the one named last changes fastest.
Arguments:
- matrix_tiles: bfloat16 [640, 128, 1024], P(('grp', 'dev')), may hold values from -0.125 to 0.125
- tile_column: int32 [640], P(('grp', 'dev')), may hold values from 0 to 255
- block_counts: int32 [256], P(('grp', 'dev')), may hold values from 1 to 4, as said below
- destination: int32 [256], P(('grp', 'dev')), may hold values from 0 to 7, as said below
- row_bounds: bfloat16 [32768], P(('grp', 'dev')), may hold values from -6 to 6
- dual_start: bfloat16 [32768], P(('grp', 'dev')), may hold values from 0 to 1
- primal_start: float32 [262144], replicated, may hold values from 0 to 0.5
- cost_vector: float32 [262144], replicated, may hold values from -6 to 6
- upper_bound: float32 [262144], replicated, may hold values from 0.5 to 2
Outputs:
- primal_final: float32 [262144], replicated
- dual_final: float32 [32768], P(('grp', 'dev'))
- weight_final: float32 [1], replicated
The draws below stay inside these ranges and needn't reach their ends.
Inputs may be any that keep to these rules, and one draw needn't show every extreme that they name: `block_counts`: each device's 8 row blocks have 1 to 4 tiles each and 20 at most together; some device has exactly 20 in every draw. `destination`: on every device the 8 entries are each of 0 to 7 once.
All inputs are finite; a program needn't handle non-finite values.
Results may differ from the reference program's by a relative error of at most 0.0015.
Values may be sent and summed in bfloat16 or wider, within the bound.
A program may use at most 128 MiB of HBM per device.

```python
import jax
import jax.numpy as jnp
from jax import lax

CB = 1024
NCB = 256
TR = 128
MAXC = 4
ITERS = 3
RB_DEV = 8
POOL_DEV = 20
RBLK = 256
ROWS = 32768
COLS = 262144
N_GRP = 4
N_DEV = 8


def layout_pair(key):
    device_count = RBLK // RB_DEV
    base_key = jax.random.fold_in(key, 7)
    key_extra, key_heavy, key_rank, key_tie = jax.random.split(base_key, 4)
    extra_tiles = jax.random.randint(key_extra, (device_count,), 0, POOL_DEV - RB_DEV + 1)
    heaviest = jax.random.randint(key_heavy, (), 0, device_count)
    extra_tiles = jnp.where(jnp.arange(device_count) == heaviest, POOL_DEV - RB_DEV, extra_tiles)
    rank_of = jax.vmap(lambda sub: jax.random.permutation(sub, RB_DEV))(jax.random.split(key_rank, device_count))
    counts = 1 + jnp.clip(extra_tiles[:, None] - rank_of * (MAXC - 1), 0, MAXC - 1)
    tie_break = jax.vmap(lambda sub: jax.random.permutation(sub, RB_DEV))(jax.random.split(key_tie, device_count))
    sorted_slots = jnp.argsort(counts * RB_DEV + tie_break, axis=1)
    position = jnp.argsort(sorted_slots, axis=1)
    member = (jnp.arange(device_count) % RB_DEV)[:, None]
    target_dev = (position + member) % RB_DEV
    return (counts.astype(jnp.int32).reshape(RBLK), target_dev.astype(jnp.int32).reshape(RBLK))


def draw_block_counts(key, part):
    return layout_pair(key)[0]


def draw_destination(key, part):
    return layout_pair(key)[1]


def plant(result, rng, low, top_value):
    longest = result.shape.index(max(result.shape))
    spots = []
    for shift in (0, 1):
        where = [jax.random.randint(jax.random.fold_in(rng, axis), (), 0, length) for axis, length in enumerate(result.shape)]
        where[longest] = (where[longest] + shift) % result.shape[longest]
        spots.append(tuple(where))
    return result.at[spots[0]].set(low).at[spots[1]].set(top_value)


def steps_of(own_key, extent, shards, low, top_value):
    level = 1.0
    for dim, blocks in shards:
        heights = jax.random.uniform(jax.random.fold_in(jax.random.fold_in(own_key, 6), dim), (blocks,), jnp.float32, low / len(shards), top_value / len(shards))
        level = level * jnp.repeat(jnp.exp(heights), extent[dim] // blocks).reshape((-1,) + (1,) * (len(extent) - 1 - dim))
    return level


def bell_draw(own_key, shape, spread, reach, cuts=(), kind=jnp.bfloat16):
    gain = steps_of(own_key, shape, cuts, -0.22, 0.18) if cuts else 1.0
    drawn = jax.random.normal(own_key, shape, jnp.float32) * spread * gain
    return jnp.minimum(jnp.maximum(drawn, -reach), reach).astype(kind)


def setup_inputs(seed: int = 0) -> dict:
    key_list = jax.random.split(jax.random.key(seed), 10)
    matrix_tiles = bell_draw(key_list[0], (N_GRP * N_DEV * POOL_DEV, TR, CB), (2 * CB) ** -0.5, 0.125, ((0, 32),))
    tile_column = plant(jax.random.randint(key_list[1], (N_GRP * N_DEV * POOL_DEV,), 0, NCB), jax.random.fold_in(key_list[1], 1), 0, NCB - 1).astype(jnp.int32)
    block_counts = draw_block_counts(jax.random.fold_in(key_list[9], 71), 0)
    destination = draw_destination(jax.random.fold_in(key_list[9], 71), 0)
    row_bounds = bell_draw(key_list[4], (ROWS,), 1.0, 6.0, ((0, 32),))
    dual_start = jnp.clip(1.0 * jax.random.uniform(key_list[5], (ROWS,), jnp.float32) ** steps_of(key_list[5], (ROWS,), ((0, 32),), -0.2, 0.2), 0.0, 1.0).astype(jnp.bfloat16)
    primal_start = jnp.clip(jax.random.uniform(key_list[6], (COLS,), jnp.float32, 0.0, 0.5), 0.0, 0.5)
    cost_vector = bell_draw(key_list[7], (COLS,), 1.0, 6.0, (), jnp.float32)
    upper_bound = jnp.clip(jax.random.uniform(key_list[8], (COLS,), jnp.float32, 0.5, 2.0), 0.5, 2.0)
    return {"matrix_tiles": matrix_tiles, "tile_column": tile_column, "block_counts": block_counts, "destination": destination, "row_bounds": row_bounds, "dual_start": dual_start, "primal_start": primal_start, "cost_vector": cost_vector, "upper_bound": upper_bound}


step_scale = 0.3

def reference(matrix_tiles, tile_column, block_counts, destination, row_bounds, dual_start, primal_start, cost_vector, upper_bound):
    device_count = N_GRP * N_DEV
    tile_set = matrix_tiles.reshape(device_count, POOL_DEV, TR, CB)
    tile_cols = tile_column.reshape(device_count, POOL_DEV)
    counts = block_counts.reshape(device_count, RB_DEV)
    starts = jnp.cumsum(counts, axis=1) - counts
    slot_ids = jnp.arange(POOL_DEV, dtype=jnp.int32)
    owners = lax.optimization_barrier(jnp.sum((starts[:, None, 1:] <= slot_ids[None, :, None]).astype(jnp.int32), axis=2))
    is_live = slot_ids[None, :] < lax.optimization_barrier(jnp.sum(counts, axis=1))[:, None]

    def apply_rows(vector_bf):
        vector_table = vector_bf.astype(jnp.float32).reshape(NCB, CB)

        def per_device(entries):
            tile_d, col_d, own_d, live_d = entries
            product = jnp.einsum('src,sc->sr', tile_d.astype(jnp.float32), vector_table[col_d], precision=lax.Precision.HIGHEST)
            product = jnp.where(live_d[:, None], product, 0.0)
            return jax.ops.segment_sum(product, own_d, num_segments=RB_DEV)
        return lax.map(per_device, (tile_set, tile_cols, owners, is_live))

    def apply_columns(rows_bf):

        def per_device(accum, entries):
            tile_d, col_d, own_d, live_d, rows_d = entries
            product = jnp.einsum('src,sr->sc', tile_d.astype(jnp.float32), rows_d.astype(jnp.float32)[own_d], precision=lax.Precision.HIGHEST)
            product = jnp.where(live_d[:, None], product, 0.0)
            return (accum + jax.ops.segment_sum(product, col_d, num_segments=NCB), None)
        accum, unused = lax.scan(per_device, jnp.zeros((NCB, CB), jnp.float32), (tile_set, tile_cols, owners, is_live, rows_bf))
        return accum.reshape(-1)
    bounds = row_bounds.astype(jnp.float32).reshape(device_count, RB_DEV, TR)
    dual_state = dual_start.astype(jnp.float32).reshape(device_count, RB_DEV, TR)
    primal = primal_start
    weight = jnp.ones((), jnp.float32)
    row_image = apply_rows(primal.astype(jnp.bfloat16))
    for iteration in range(ITERS):
        step_primal = step_scale / weight
        step_dual = step_scale * weight
        gradient = apply_columns(dual_state.astype(jnp.bfloat16))
        primal_next = jnp.clip(primal - step_primal * (cost_vector - gradient), 0.0, upper_bound)
        change = jnp.sum((primal_next - primal) ** 2)
        next_image = apply_rows(primal_next.astype(jnp.bfloat16))
        dual_state = jnp.maximum(dual_state + step_dual * (bounds - (2.0 * next_image - row_image)), 0.0)
        violation = jnp.sum(jnp.maximum(bounds - next_image, 0.0) ** 2)
        weight = jnp.sqrt(weight * jnp.sqrt((violation + 1e-06) / (change + 1e-06)))
        primal = primal_next
        row_image = next_image
    grouped = dual_state.reshape(N_GRP, N_DEV, RB_DEV, TR)
    target = destination.reshape(N_GRP, N_DEV, RB_DEV)
    group_index = jnp.broadcast_to(jnp.arange(N_GRP, dtype=jnp.int32)[:, None, None], target.shape)
    member_index = jnp.broadcast_to(jnp.arange(N_DEV, dtype=jnp.int32)[None, :, None], target.shape)
    placed = jnp.zeros((N_GRP, N_DEV, N_DEV, TR), jnp.float32).at[group_index, target, member_index].set(grouped)
    return (primal, placed.reshape(-1), jnp.reshape(weight, (1,)))
```

```python
import functools

import jax
import jax.numpy as jnp
from jax import lax
from jax.experimental import pallas as pl
from jax.experimental.pallas import tpu as pltpu
from jax.sharding import PartitionSpec as P

NCB = 256
ITERS = 3


step_scale = 0.3


def row_products(tile_store, vector_bf, blocks):
    tile_set, tile_cols, owners, live_flags = tile_store
    vector_table = vector_bf.reshape(-1, tile_set.shape[2])
    column_hot = (
        tile_cols[:, None] == jnp.arange(vector_table.shape[0], dtype=jnp.int32)[None, :]
    ).astype(jnp.bfloat16)
    picked = jnp.dot(column_hot, vector_table, preferred_element_type=jnp.float32).astype(
        jnp.bfloat16
    )
    product = jnp.einsum("src,sc->sr", tile_set, picked, preferred_element_type=jnp.float32)
    product = jnp.where(live_flags[:, None], product, 0.0)
    owner_hot = (jnp.arange(blocks, dtype=jnp.int32)[:, None] == owners[None, :]).astype(
        jnp.float32
    )
    return jnp.dot(owner_hot, product, precision=lax.Precision.HIGHEST)


def column_products(tile_store, rows_bf):
    tile_set, tile_cols, owners, live_flags = tile_store
    blocks = rows_bf.shape[0]
    owner_hot = (owners[:, None] == jnp.arange(blocks, dtype=jnp.int32)[None, :]).astype(
        jnp.bfloat16
    )
    picked_rows = jnp.dot(owner_hot, rows_bf, preferred_element_type=jnp.float32).astype(
        jnp.bfloat16
    )
    product = jnp.einsum("src,sr->sc", tile_set, picked_rows, preferred_element_type=jnp.float32)
    product = jnp.where(live_flags[:, None], product, 0.0)
    column_hot = (jnp.arange(NCB, dtype=jnp.int32)[:, None] == tile_cols[None, :]).astype(
        jnp.float32
    )
    return jnp.dot(column_hot, product, precision=lax.Precision.HIGHEST).reshape(-1)


def per_device(
    matrix_tiles,
    tile_column,
    block_counts,
    destination,
    row_bounds,
    dual_start,
    primal_start,
    cost_vector,
    upper_bound,
):
    blocks = block_counts.shape[0]
    rows_per = matrix_tiles.shape[1]
    slot_count = matrix_tiles.shape[0]
    starts = jnp.cumsum(block_counts) - block_counts
    slot_ids = jnp.arange(slot_count, dtype=jnp.int32)
    owners = jnp.sum((starts[None, 1:] <= slot_ids[:, None]).astype(jnp.int32), axis=1)
    bounds_here = row_bounds.reshape(blocks, rows_per)
    dual_here = dual_start.reshape(blocks, rows_per)
    peer_ids = jnp.arange(blocks, dtype=jnp.int32)
    inverse = jnp.sum(
        jnp.where(destination[None, :] == peer_ids[:, None], peer_ids[None, :], 0), axis=1
    )
    tile_store = (matrix_tiles, tile_column, owners, slot_ids < jnp.sum(block_counts))
    bounds = bounds_here.astype(jnp.float32)
    dual_state = dual_here.astype(jnp.float32)
    primal = primal_start
    weight = jnp.ones((), jnp.float32)
    row_image = row_products(tile_store, primal.astype(jnp.bfloat16), blocks)
    for iteration in range(ITERS):
        step_primal = step_scale / weight
        step_dual = step_scale * weight
        partial_value = column_products(tile_store, dual_state.astype(jnp.bfloat16))
        gradient = lax.psum(partial_value, ("grp", "dev"))
        primal_next = jnp.clip(primal - step_primal * (cost_vector - gradient), 0.0, upper_bound)
        change = jnp.sum((primal_next - primal) ** 2)
        next_image = row_products(tile_store, primal_next.astype(jnp.bfloat16), blocks)
        dual_state = jnp.maximum(
            dual_state + step_dual * (bounds - (2.0 * next_image - row_image)), 0.0
        )
        violation_part = jnp.sum(jnp.maximum(bounds - next_image, 0.0) ** 2)
        violation = lax.psum(violation_part, ("grp", "dev"))
        weight = jnp.sqrt(weight * jnp.sqrt((violation + 1e-06) / (change + 1e-06)))
        primal = primal_next
        row_image = next_image
    dual_final = lax.all_to_all(
        dual_state[inverse], "dev", split_axis=0, concat_axis=0, tiled=True
    ).reshape(-1)
    return (primal, dual_final, jnp.reshape(weight, (1,)))


MESH_ID = pl.DeviceIdType.MESH
SPLIT = 4


def tile_split(slot_count):
    main = slot_count // 16 * 16
    return main, (slot_count - main) * SPLIT


def fits(mesh_shape, slot_count, rows_per, width, blocks, column_blocks):
    main, tail = tile_split(slot_count)
    devices = mesh_shape["grp"] * mesh_shape["dev"]
    rows = main + tail
    per_group = 128
    if main == 0 or per_group % main or rows > 96 or slot_count % 4:
        return False
    if tail == 0 or per_group % tail or tail % 16:
        return False
    if (devices * main) % 128 or (devices * tail) % 128:
        return False
    if rows_per != 128 or width % (128 * SPLIT) or blocks != mesh_shape["dev"]:
        return False
    if mesh_shape["dev"] % 2 or column_blocks > 256 or column_blocks % 16:
        return False
    held = slot_count * rows_per * width * 2 + 2 * devices * rows * width * 2
    return held < 30 * 2**20


def fused_kernel(
    n_grp,
    n_dev,
    cols,
    counts,
    dest,
    rows_in,
    tiles,
    primal_in,
    cost_in,
    upper_in,
    out_primal,
    out_dual,
    out_weight,
    kv,
    pv,
    cv,
    uv,
    pnow,
    pbf,
    hot,
    buf,
    stat,
    dsend,
    drecv,
    local_sem,
    piece_send,
    piece_recv,
    stat_send,
    stat_recv,
    dual_send,
    dual_recv,
):
    slots, rows_per, width = tiles.shape
    blocks = counts.shape[0]
    n_cb = pnow.shape[0]
    n_all = n_grp * n_dev
    n_chip = n_dev // 2
    main, tail = tile_split(slots)
    rest = slots - main
    rows = main + tail
    sub = width // SPLIT
    chunks = width // 128
    g = lax.axis_index("grp")
    d = lax.axis_index("dev")
    core = d % 2
    chip = d // 2
    partner = chip * 2 + (1 - core)
    me = g * n_dev + d
    f32, bf16, i32 = jnp.float32, jnp.bfloat16, jnp.int32

    def remote(src, dst, ssem, rsem, tg, td):
        return pltpu.make_async_remote_copy(
            src_ref=src,
            dst_ref=dst,
            send_sem=ssem,
            recv_sem=rsem,
            device_id={"grp": tg, "dev": td},
            device_id_type=MESH_ID,
        )

    others = [(a, b) for a in range(n_grp) for b in range(n_dev) if a or b]

    def other(a, b):
        return (g + a) % n_grp, (d + b) % n_dev

    barrier = pltpu.get_barrier_semaphore()
    for a, b in others:
        tg, td = other(a, b)
        pl.semaphore_signal(
            barrier, inc=1, device_id={"grp": tg, "dev": td}, device_id_type=MESH_ID
        )
    copies = [
        pltpu.make_async_copy(primal_in, pv, local_sem.at[0]),
        pltpu.make_async_copy(cost_in, cv, local_sem.at[1]),
        pltpu.make_async_copy(upper_in, uv, local_sem.at[2]),
    ]
    part = slots // 4
    for k in range(4):
        copies.append(
            pltpu.make_async_copy(
                tiles.at[pl.ds(k * part, part)], kv.at[pl.ds(k * part, part)], local_sem.at[3 + k]
            )
        )
    copies[0].start()
    for k in range(4):
        copies[3 + k].start()
    copies[1].start()
    copies[2].start()

    def slot_of(pos):
        return jnp.where(pos < main, pos, main + (pos - main) % rest)

    starts = [counts[0] * 0]
    for b in range(blocks):
        starts.append(starts[-1] + counts[b])
    total = starts[-1]
    lane = lax.broadcasted_iota(i32, (1, 128), 1)
    lane_slot = jnp.where(lane < rows, slot_of(lane), slots)
    row = lax.broadcasted_iota(i32, (rows, 128), 0)
    row_slot = slot_of(row)
    row_wide = lax.broadcasted_iota(i32, (rows, n_cb), 0)
    wide_slot = slot_of(row_wide)
    stat_row = jnp.full((1, 128), -1.0, f32)
    wide_col = jnp.full((rows, n_cb), -1, i32)
    owner_of = []
    for s in range(slots):
        live_col = jnp.where(s < total, cols[s], -1)
        stat_row = jnp.where(lane_slot == s, live_col.astype(f32), stat_row)
        wide_col = jnp.where(wide_slot == s, live_col, wide_col)
        who = jnp.int32(0)
        for b in range(1, blocks):
            who = who + jnp.where(starts[b] <= s, 1, 0)
        owner_of.append(jnp.where(s < total, who, -1))
    own_hot = jnp.where(
        wide_col == lax.broadcasted_iota(i32, (rows, n_cb), 1), 1.0, 0.0
    ).astype(bf16)
    row_owner = jnp.zeros((rows, 128), i32)
    for b in range(1, blocks):
        row_owner = row_owner + jnp.where(row_slot >= starts[b], 1, 0)
    row_owner = jnp.where(row_slot < total, row_owner, -1)
    block_row = lax.broadcasted_iota(i32, (blocks, 128), 0)
    bounds = rows_in[0]
    dual = rows_in[1]

    stat[0, me] = stat_row
    pl.semaphore_wait(barrier, len(others))

    def send_stat(turn):
        sent = []
        for k, (a, b) in enumerate(others):
            tg, td = other(a, b)
            copy = remote(
                stat.at[turn, me],
                stat.at[turn, me],
                stat_send.at[turn, k],
                stat_recv.at[turn, me],
                tg,
                td,
            )
            copy.start()
            sent.append(copy)
        return sent

    def wait_stat(turn):
        for a, b in others:
            tg, td = other(a, b)
            src = tg * n_dev + td
            remote(
                stat.at[turn, src],
                stat.at[turn, src],
                stat_send.at[turn, 0],
                stat_recv.at[turn, src],
                tg,
                td,
            ).wait_recv()

    pending = send_stat(0)

    def row_image_of():
        picked = jnp.dot(own_hot, pbf[...], preferred_element_type=f32).astype(bf16)
        chosen = jnp.zeros((rows, rows_per), f32)
        for s in range(0, slots, 2):
            pair = kv[s : s + 2].reshape(2 * rows_per, width)
            both = lax.dot_general(
                picked, pair, (((1,), (1,)), ((), ())), preferred_element_type=f32
            )
            chosen = jnp.where(row == s, both[:, :rows_per], chosen)
            chosen = jnp.where(row == s + 1, both[:, rows_per:], chosen)
        image = jnp.zeros((blocks, rows_per), f32)
        for s in range(slots):
            image = image + jnp.where(block_row == owner_of[s], chosen[s : s + 1, :], 0.0)
        return image

    def write_piece(p, dual_now):
        spread = jnp.zeros((rows, rows_per), f32)
        for b in range(blocks):
            spread = jnp.where(row_owner == b, dual_now[b : b + 1, :], spread)
        total_piece = jnp.zeros((rows, width), f32)
        for s in range(0, slots, 2):
            left = jnp.concatenate(
                [
                    jnp.where(row_slot == s, spread, 0.0),
                    jnp.where(row_slot == s + 1, spread, 0.0),
                ],
                axis=1,
            ).astype(bf16)
            pair = kv[s : s + 2].reshape(2 * rows_per, width)
            total_piece = total_piece + jnp.dot(left, pair, preferred_element_type=f32)
        quarter = lax.broadcasted_iota(i32, (tail, sub), 0) // rest
        ends = jnp.zeros((tail, sub), f32)
        for q in range(SPLIT):
            part_q = total_piece[:, q * sub : (q + 1) * sub]
            buf[p, me, q * main : (q + 1) * main, :] = part_q[:main].astype(bf16)
            ends = jnp.where(quarter == q, part_q[main:], ends)
        buf[p, me, SPLIT * main : SPLIT * main + tail, :] = ends.astype(bf16)

    def exchange(p, middle):
        sent = []

        def send(slot, tg, td):
            copy = remote(
                buf.at[p, slot],
                buf.at[p, slot],
                piece_send.at[len(sent)],
                piece_recv.at[p, slot],
                tg,
                td,
            )
            copy.start()
            sent.append(copy)

        def arrived(slot):
            remote(
                buf.at[p, slot],
                buf.at[p, slot],
                piece_send.at[0],
                piece_recv.at[p, slot],
                g,
                partner,
            ).wait_recv()

        def plane(slot):
            for k in range(1, n_chip):
                send(slot, g, ((chip + k) % n_chip) * 2 + core)
            send(slot, g, partner)

        for a in range(1, n_grp):
            send(me, (g + a) % n_grp, d)
        plane(me)
        middle()
        order = sorted(range(1, n_grp), key=lambda a: min(a, n_grp - a))
        for a in order:
            slot = ((g + a) % n_grp) * n_dev + d
            arrived(slot)
            plane(slot)
        for a in [0] + order:
            for k in range(1, n_chip):
                slot = ((g + a) % n_grp) * n_dev + ((chip + k) % n_chip) * 2 + core
                arrived(slot)
                send(slot, g, partner)
        for a in [0] + order:
            for k in range(n_chip):
                arrived(((g + a) % n_grp) * n_dev + ((chip + k) % n_chip) * 2 + (1 - core))
        return sent

    def build_hot():
        wait_stat(0)
        block_of = lax.broadcasted_iota(i32, (n_cb, 128), 0).astype(f32)
        for base, size, start in ((0, main, 0), (main, tail, n_all * main)):
            per = 128 // size
            for group in range(n_all // per):
                line = jnp.full((1, 128), -1.0, f32)
                for k in range(per):
                    shift = (k * size - base) % 128
                    source = stat[0, group * per + k]
                    moved = source if shift == 0 else pltpu.roll(source, shift, 1)
                    line = jnp.where(lane // size == k, moved, line)
                match = jnp.where(block_of == line, 1.0, 0.0)
                if base == 0:
                    hot[:, group * 128 : (group + 1) * 128] = match.astype(bf16)
                else:
                    for q in range(SPLIT):
                        at = start + q * n_all * tail + group * 128
                        keep = jnp.where((lane % size) // rest == q, match, 0.0)
                        hot[:, at : at + 128] = keep.astype(bf16)

    copies[0].wait()
    for j in range(chunks):
        value = pv[pl.ds(j, n_cb, stride=chunks), :]
        pnow[:, j * 128 : (j + 1) * 128] = value
        pbf[:, j * 128 : (j + 1) * 128] = value.astype(bf16)
    for k in range(4):
        copies[3 + k].wait()

    weight = jnp.ones((1, 1), f32)
    change = None
    image = None
    for it in range(ITERS):
        p = it % 2
        write_piece(p, dual)
        if it == 0:

            def first():
                build_hot()

            sent = exchange(p, first)
            image = row_image_of()
            copies[1].wait()
            copies[2].wait()
        else:
            sent = exchange(p, lambda: None)
            wait_stat(it)
            violation = jnp.sum(stat[it], axis=0)[:, 127:128]
            weight = jnp.sqrt(weight * jnp.sqrt((violation + 1e-06) / (change + 1e-06)))
        tau = step_scale / weight
        ends = buf[p, :, SPLIT * main :, :].reshape(n_all * tail, sub)
        moved_sum = jnp.zeros((8, 128), f32)
        for q in range(SPLIT):
            body = buf[p, :, q * main : (q + 1) * main, :].reshape(n_all * main, sub)
            at = n_all * main + q * n_all * tail
            grad = jnp.dot(hot[:, : n_all * main], body, preferred_element_type=f32)
            grad = grad + jnp.dot(
                hot[:, at : at + n_all * tail], ends, preferred_element_type=f32
            )
            for h in range(sub // 128):
                j = q * (sub // 128) + h
                here = pl.ds(j, n_cb, stride=chunks)
                span = slice(j * 128, (j + 1) * 128)
                old = pnow[:, span]
                stepped = old - tau * (cv[here, :] - grad[:, h * 128 : (h + 1) * 128])
                new = jnp.minimum(jnp.maximum(stepped, 0.0), uv[here, :])
                gap = new - old
                moved_sum = moved_sum + jnp.sum((gap * gap).reshape(n_cb // 8, 8, 128), axis=0)
                pnow[:, span] = new
                pbf[:, span] = new.astype(bf16)
                if it == ITERS - 1:
                    out_primal[here, :] = new
        change = jnp.sum(moved_sum, axis=(0, 1), keepdims=True)
        next_image = row_image_of()
        sigma = step_scale * weight
        dual = jnp.maximum(dual + sigma * (bounds - (2.0 * next_image - image)), 0.0)
        short = jnp.maximum(bounds - next_image, 0.0)
        image = next_image
        stat[it + 1, me] = jnp.where(
            lane == 127, jnp.sum(short * short, axis=(0, 1), keepdims=True), 0.0
        )
        for copy in pending:
            copy.wait_send()
        for copy in sent:
            copy.wait_send()
        pending = send_stat(it + 1)

    for e in range(n_dev):
        line = jnp.zeros((1, rows_per), f32)
        for k in range(blocks):
            line = jnp.where(dest[k] == e, dual[k : k + 1, :], line)
        dsend[e] = line
    sent = []
    for k in range(1, n_dev):
        td = (d + k) % n_dev
        copy = remote(dsend.at[td], drecv.at[d], dual_send.at[k], dual_recv.at[d], g, td)
        copy.start()
        sent.append(copy)
    drecv[d] = dsend[d]
    wait_stat(ITERS)
    violation = jnp.sum(stat[ITERS], axis=0)[:, 127:128]
    weight = jnp.sqrt(weight * jnp.sqrt((violation + 1e-06) / (change + 1e-06)))
    out_weight[...] = jnp.broadcast_to(weight, (1, 128))
    for k in range(1, n_dev):
        src = (d + k) % n_dev
        remote(dsend.at[src], drecv.at[src], dual_send.at[k], dual_recv.at[src], g, src).wait_recv()
    out_dual[...] = drecv[...]
    for copy in pending:
        copy.wait_send()
    for copy in sent:
        copy.wait_send()


def fused_device(mesh_shape, *args):
    tiles, cols, counts, dest, row_bounds, dual_start, primal, cost, upper = args
    slots, rows_per, width = tiles.shape
    blocks = counts.shape[0]
    column_blocks = primal.shape[0] // width
    if not fits(mesh_shape, slots, rows_per, width, blocks, column_blocks):
        return per_device(*args)
    n_grp, n_dev = mesh_shape["grp"], mesh_shape["dev"]
    n_all = n_grp * n_dev
    main, tail = tile_split(slots)
    rows_in = (
        jnp.stack([row_bounds, dual_start]).astype(jnp.float32).reshape(2, blocks, rows_per)
    )
    flat = (primal.shape[0] // 128, 128)
    f32, bf16 = jnp.float32, jnp.bfloat16
    vmem = pl.BlockSpec(memory_space=pltpu.VMEM)
    smem = pl.BlockSpec(memory_space=pltpu.SMEM)
    anywhere = pl.BlockSpec(memory_space=pl.ANY)
    sends = (n_grp - 1) + n_grp * (n_dev // 2) + n_grp * (n_dev // 2 - 1)
    out_primal, out_dual, out_weight = pl.pallas_call(
        functools.partial(fused_kernel, n_grp, n_dev),
        name="pdhg_fused",
        out_shape=(
            jax.ShapeDtypeStruct(flat, f32),
            jax.ShapeDtypeStruct((n_dev, 1, rows_per), f32),
            jax.ShapeDtypeStruct((1, 128), f32),
        ),
        in_specs=[smem, smem, smem, vmem, anywhere, anywhere, anywhere, anywhere],
        out_specs=(vmem, vmem, vmem),
        scratch_shapes=[
            pltpu.VMEM((slots, rows_per, width), bf16),
            pltpu.VMEM(flat, f32),
            pltpu.VMEM(flat, f32),
            pltpu.VMEM(flat, f32),
            pltpu.VMEM((column_blocks, width), f32),
            pltpu.VMEM((column_blocks, width), bf16),
            pltpu.VMEM((column_blocks, n_all * (main + SPLIT * tail)), bf16),
            pltpu.VMEM((2, n_all, SPLIT * main + tail, width // SPLIT), bf16),
            pltpu.VMEM((ITERS + 1, n_all, 1, 128), f32),
            pltpu.VMEM((n_dev, 1, rows_per), f32),
            pltpu.VMEM((n_dev, 1, rows_per), f32),
            pltpu.SemaphoreType.DMA((7,)),
            pltpu.SemaphoreType.DMA((sends,)),
            pltpu.SemaphoreType.DMA((2, n_all)),
            pltpu.SemaphoreType.DMA((ITERS + 1, n_all)),
            pltpu.SemaphoreType.DMA((ITERS + 1, n_all)),
            pltpu.SemaphoreType.DMA((n_dev,)),
            pltpu.SemaphoreType.DMA((n_dev,)),
        ],
        compiler_params=pltpu.CompilerParams(
            collective_id=0, has_side_effects=True, vmem_limit_bytes=48 * 2**20
        ),
    )(
        cols,
        counts,
        dest,
        rows_in,
        tiles,
        primal.reshape(flat),
        cost.reshape(flat),
        upper.reshape(flat),
    )
    return out_primal.reshape(-1), out_dual.reshape(-1), out_weight[0, :1]


def solution(mesh):
    in_specs = (
        P(("grp", "dev"), None, None),
        P(("grp", "dev")),
        P(("grp", "dev")),
        P(("grp", "dev")),
        P(("grp", "dev")),
        P(("grp", "dev")),
        P(),
        P(),
        P(),
    )
    out_specs = (P(), P(("grp", "dev")), P())
    return jax.shard_map(
        functools.partial(fused_device, dict(mesh.shape)),
        mesh=mesh,
        in_specs=in_specs,
        out_specs=out_specs,
        check_vma=False,
    )
```

```python
import functools

import jax
import jax.numpy as jnp
from jax import lax
from jax.experimental import pallas as pl
from jax.experimental.pallas import tpu as pltpu
from jax.sharding import PartitionSpec as P

NCB = 256
ITERS = 3


step_scale = 0.3


def row_products(tile_store, vector_bf, blocks):
    tile_set, tile_cols, owners, live_flags = tile_store
    vector_table = vector_bf.reshape(-1, tile_set.shape[2])
    column_hot = (
        tile_cols[:, None] == jnp.arange(vector_table.shape[0], dtype=jnp.int32)[None, :]
    ).astype(jnp.bfloat16)
    picked = jnp.dot(column_hot, vector_table, preferred_element_type=jnp.float32).astype(
        jnp.bfloat16
    )
    product = jnp.einsum("src,sc->sr", tile_set, picked, preferred_element_type=jnp.float32)
    product = jnp.where(live_flags[:, None], product, 0.0)
    owner_hot = (jnp.arange(blocks, dtype=jnp.int32)[:, None] == owners[None, :]).astype(
        jnp.float32
    )
    return jnp.dot(owner_hot, product, precision=lax.Precision.HIGHEST)


def column_products(tile_store, rows_bf):
    tile_set, tile_cols, owners, live_flags = tile_store
    blocks = rows_bf.shape[0]
    owner_hot = (owners[:, None] == jnp.arange(blocks, dtype=jnp.int32)[None, :]).astype(
        jnp.bfloat16
    )
    picked_rows = jnp.dot(owner_hot, rows_bf, preferred_element_type=jnp.float32).astype(
        jnp.bfloat16
    )
    product = jnp.einsum("src,sr->sc", tile_set, picked_rows, preferred_element_type=jnp.float32)
    product = jnp.where(live_flags[:, None], product, 0.0)
    column_hot = (jnp.arange(NCB, dtype=jnp.int32)[:, None] == tile_cols[None, :]).astype(
        jnp.float32
    )
    return jnp.dot(column_hot, product, precision=lax.Precision.HIGHEST).reshape(-1)


def per_device(
    matrix_tiles,
    tile_column,
    block_counts,
    destination,
    row_bounds,
    dual_start,
    primal_start,
    cost_vector,
    upper_bound,
):
    blocks = block_counts.shape[0]
    rows_per = matrix_tiles.shape[1]
    slot_count = matrix_tiles.shape[0]
    starts = jnp.cumsum(block_counts) - block_counts
    slot_ids = jnp.arange(slot_count, dtype=jnp.int32)
    owners = jnp.sum((starts[None, 1:] <= slot_ids[:, None]).astype(jnp.int32), axis=1)
    bounds_here = row_bounds.reshape(blocks, rows_per)
    dual_here = dual_start.reshape(blocks, rows_per)
    peer_ids = jnp.arange(blocks, dtype=jnp.int32)
    inverse = jnp.sum(
        jnp.where(destination[None, :] == peer_ids[:, None], peer_ids[None, :], 0), axis=1
    )
    tile_store = (matrix_tiles, tile_column, owners, slot_ids < jnp.sum(block_counts))
    bounds = bounds_here.astype(jnp.float32)
    dual_state = dual_here.astype(jnp.float32)
    primal = primal_start
    weight = jnp.ones((), jnp.float32)
    row_image = row_products(tile_store, primal.astype(jnp.bfloat16), blocks)
    for iteration in range(ITERS):
        step_primal = step_scale / weight
        step_dual = step_scale * weight
        partial_value = column_products(tile_store, dual_state.astype(jnp.bfloat16))
        gradient = lax.psum(partial_value, ("grp", "dev"))
        primal_next = jnp.clip(primal - step_primal * (cost_vector - gradient), 0.0, upper_bound)
        change = jnp.sum((primal_next - primal) ** 2)
        next_image = row_products(tile_store, primal_next.astype(jnp.bfloat16), blocks)
        dual_state = jnp.maximum(
            dual_state + step_dual * (bounds - (2.0 * next_image - row_image)), 0.0
        )
        violation_part = jnp.sum(jnp.maximum(bounds - next_image, 0.0) ** 2)
        violation = lax.psum(violation_part, ("grp", "dev"))
        weight = jnp.sqrt(weight * jnp.sqrt((violation + 1e-06) / (change + 1e-06)))
        primal = primal_next
        row_image = next_image
    dual_final = lax.all_to_all(
        dual_state[inverse], "dev", split_axis=0, concat_axis=0, tiled=True
    ).reshape(-1)
    return (primal, dual_final, jnp.reshape(weight, (1,)))


MESH_ID = pl.DeviceIdType.MESH
SPLIT = 4


def tile_split(slot_count):
    main = slot_count // 16 * 16
    return main, (slot_count - main) * SPLIT


def fits(mesh_shape, slot_count, rows_per, width, blocks, column_blocks):
    main, tail = tile_split(slot_count)
    devices = mesh_shape["grp"] * mesh_shape["dev"]
    rows = main + tail
    per_group = 128
    if main == 0 or per_group % main or rows > 96 or slot_count % 4:
        return False
    if tail == 0 or per_group % tail or tail % 16:
        return False
    if (devices * main) % 128 or (devices * tail) % 128:
        return False
    if rows_per != 128 or width % (128 * SPLIT) or blocks != mesh_shape["dev"]:
        return False
    if mesh_shape["dev"] % 2 or column_blocks > 256 or column_blocks % 16:
        return False
    held = slot_count * rows_per * width * 2 + 2 * devices * rows * width * 2
    return held < 30 * 2**20


def fused_kernel(
    n_grp,
    n_dev,
    indices,
    rows_in,
    tiles,
    primal_in,
    cost_in,
    upper_in,
    out_primal,
    out_dual,
    out_weight,
    kv,
    pv,
    cv,
    uv,
    pnow,
    pbf,
    hot,
    buf,
    stat,
    dsend,
    drecv,
    local_sem,
    piece_send,
    piece_recv,
    stat_send,
    stat_recv,
    dual_send,
    dual_recv,
):
    slots, rows_per, width = tiles.shape
    blocks = rows_in.shape[1]
    cols = [indices[k] for k in range(slots)]
    counts = [indices[slots + k] for k in range(blocks)]
    dest = [indices[slots + blocks + k] for k in range(blocks)]
    n_cb = pnow.shape[0]
    n_all = n_grp * n_dev
    n_chip = n_dev // 2
    main, tail = tile_split(slots)
    rest = slots - main
    rows = main + tail
    sub = width // SPLIT
    chunks = width // 128
    g = lax.axis_index("grp")
    d = lax.axis_index("dev")
    core = d % 2
    chip = d // 2
    partner = chip * 2 + (1 - core)
    me = g * n_dev + d
    f32, bf16, i32 = jnp.float32, jnp.bfloat16, jnp.int32

    def remote(src, dst, ssem, rsem, tg, td):
        return pltpu.make_async_remote_copy(
            src_ref=src,
            dst_ref=dst,
            send_sem=ssem,
            recv_sem=rsem,
            device_id={"grp": tg, "dev": td},
            device_id_type=MESH_ID,
        )

    others = [(a, b) for a in range(n_grp) for b in range(n_dev) if a or b]

    def other(a, b):
        return (g + a) % n_grp, (d + b) % n_dev

    barrier = pltpu.get_barrier_semaphore()
    for a, b in others:
        tg, td = other(a, b)
        pl.semaphore_signal(
            barrier, inc=1, device_id={"grp": tg, "dev": td}, device_id_type=MESH_ID
        )
    copies = [
        pltpu.make_async_copy(primal_in, pv, local_sem.at[0]),
        pltpu.make_async_copy(cost_in, cv, local_sem.at[1]),
        pltpu.make_async_copy(upper_in, uv, local_sem.at[2]),
    ]
    part = 4
    parts = slots // part
    for k in range(parts):
        copies.append(
            pltpu.make_async_copy(
                tiles.at[pl.ds(k * part, part)], kv.at[pl.ds(k * part, part)], local_sem.at[3 + k]
            )
        )
    for k in range(parts):
        copies[3 + k].start()
    copies[0].start()
    copies[1].start()
    copies[2].start()

    def slot_of(pos):
        return jnp.where(pos < main, pos, main + (pos - main) % rest)

    starts = [counts[0] * 0]
    for b in range(blocks):
        starts.append(starts[-1] + counts[b])
    total = starts[-1]
    lane = lax.broadcasted_iota(i32, (1, 128), 1)
    lane_slot = jnp.where(lane < rows, slot_of(lane), slots)
    row = lax.broadcasted_iota(i32, (rows, 128), 0)
    row_slot = slot_of(row)
    row_wide = lax.broadcasted_iota(i32, (rows, n_cb), 0)
    wide_slot = slot_of(row_wide)
    stat_row = jnp.full((1, 128), -1.0, f32)
    wide_col = jnp.full((rows, n_cb), -1, i32)
    owner_of = []
    for s in range(slots):
        live_col = jnp.where(s < total, cols[s], -1)
        stat_row = jnp.where(lane_slot == s, live_col.astype(f32), stat_row)
        wide_col = jnp.where(wide_slot == s, live_col, wide_col)
        who = jnp.int32(0)
        for b in range(1, blocks):
            who = who + jnp.where(starts[b] <= s, 1, 0)
        owner_of.append(jnp.where(s < total, who, -1))
    own_hot = jnp.where(
        wide_col == lax.broadcasted_iota(i32, (rows, n_cb), 1), 1.0, 0.0
    ).astype(bf16)
    row_owner = jnp.zeros((rows, 128), i32)
    for b in range(1, blocks):
        row_owner = row_owner + jnp.where(row_slot >= starts[b], 1, 0)
    row_owner = jnp.where(row_slot < total, row_owner, -1)
    block_row = lax.broadcasted_iota(i32, (blocks, 128), 0)
    bounds = rows_in[0]
    dual = rows_in[1]

    stat[0, me] = stat_row
    pl.semaphore_wait(barrier, len(others))

    def send_stat(turn):
        sent = []
        for k, (a, b) in enumerate(others):
            tg, td = other(a, b)
            copy = remote(
                stat.at[turn, me],
                stat.at[turn, me],
                stat_send.at[turn, k],
                stat_recv.at[turn, me],
                tg,
                td,
            )
            copy.start()
            sent.append(copy)
        return sent

    def wait_stat(turn):
        for a, b in others:
            tg, td = other(a, b)
            src = tg * n_dev + td
            remote(
                stat.at[turn, src],
                stat.at[turn, src],
                stat_send.at[turn, 0],
                stat_recv.at[turn, src],
                tg,
                td,
            ).wait_recv()

    pending = send_stat(0)

    def row_image_of():
        picked = jnp.dot(own_hot, pbf[...], preferred_element_type=f32).astype(bf16)
        chosen = jnp.zeros((rows, rows_per), f32)
        for s in range(0, slots, 2):
            pair = kv[s : s + 2].reshape(2 * rows_per, width)
            both = lax.dot_general(
                picked, pair, (((1,), (1,)), ((), ())), preferred_element_type=f32
            )
            chosen = jnp.where(row == s, both[:, :rows_per], chosen)
            chosen = jnp.where(row == s + 1, both[:, rows_per:], chosen)
        image = jnp.zeros((blocks, rows_per), f32)
        for s in range(slots):
            image = image + jnp.where(block_row == owner_of[s], chosen[s : s + 1, :], 0.0)
        return image

    def write_piece(p, dual_now, loading):
        spread = jnp.zeros((rows, rows_per), f32)
        for b in range(blocks):
            spread = jnp.where(row_owner == b, dual_now[b : b + 1, :], spread)
        total_piece = jnp.zeros((rows, width), f32)
        for s in range(0, slots, 2):
            if loading and s % part == 0:
                copies[3 + s // part].wait()
            left = jnp.concatenate(
                [
                    jnp.where(row_slot == s, spread, 0.0),
                    jnp.where(row_slot == s + 1, spread, 0.0),
                ],
                axis=1,
            ).astype(bf16)
            pair = kv[s : s + 2].reshape(2 * rows_per, width)
            total_piece = total_piece + jnp.dot(left, pair, preferred_element_type=f32)
        quarter = lax.broadcasted_iota(i32, (tail, sub), 0) // rest
        ends = jnp.zeros((tail, sub), f32)
        for q in range(SPLIT):
            part_q = total_piece[:, q * sub : (q + 1) * sub]
            buf[p, me, q * main : (q + 1) * main, :] = part_q[:main].astype(bf16)
            ends = jnp.where(quarter == q, part_q[main:], ends)
        buf[p, me, SPLIT * main : SPLIT * main + tail, :] = ends.astype(bf16)

    def exchange(p, middle, later):
        sent = []

        def send(slot, tg, td):
            copy = remote(
                buf.at[p, slot],
                buf.at[p, slot],
                piece_send.at[len(sent)],
                piece_recv.at[p, slot],
                tg,
                td,
            )
            copy.start()
            sent.append(copy)

        def arrived(slot):
            remote(
                buf.at[p, slot],
                buf.at[p, slot],
                piece_send.at[0],
                piece_recv.at[p, slot],
                g,
                partner,
            ).wait_recv()

        def plane(slot):
            for k in range(1, n_chip):
                send(slot, g, ((chip + k) % n_chip) * 2 + core)
            send(slot, g, partner)

        for a in range(1, n_grp):
            send(me, (g + a) % n_grp, d)
        plane(me)
        middle()
        order = sorted(range(1, n_grp), key=lambda a: min(a, n_grp - a))
        for a in order:
            slot = ((g + a) % n_grp) * n_dev + d
            arrived(slot)
            plane(slot)
        later()
        for a in [0] + order:
            for k in range(1, n_chip):
                slot = ((g + a) % n_grp) * n_dev + ((chip + k) % n_chip) * 2 + core
                arrived(slot)
                send(slot, g, partner)
        for a in [0] + order:
            for k in range(n_chip):
                arrived(((g + a) % n_grp) * n_dev + ((chip + k) % n_chip) * 2 + (1 - core))
        return sent

    def build_hot():
        wait_stat(0)
        block_of = lax.broadcasted_iota(i32, (n_cb, 128), 0).astype(f32)
        for base, size, start in ((0, main, 0), (main, tail, n_all * main)):
            per = 128 // size
            for group in range(n_all // per):
                line = jnp.full((1, 128), -1.0, f32)
                for k in range(per):
                    shift = (k * size - base) % 128
                    source = stat[0, group * per + k]
                    moved = source if shift == 0 else pltpu.roll(source, shift, 1)
                    line = jnp.where(lane // size == k, moved, line)
                match = jnp.where(block_of == line, 1.0, 0.0)
                if base == 0:
                    hot[:, group * 128 : (group + 1) * 128] = match.astype(bf16)
                else:
                    for q in range(SPLIT):
                        at = start + q * n_all * tail + group * 128
                        keep = jnp.where((lane % size) // rest == q, match, 0.0)
                        hot[:, at : at + 128] = keep.astype(bf16)

    weight = jnp.ones((1, 1), f32)
    change = None
    image = None
    for it in range(ITERS):
        p = it % 2
        write_piece(p, dual, it == 0)
        if it == 0:

            images = []

            def first():
                copies[0].wait()
                for j in range(chunks):
                    value = pv[pl.ds(j, n_cb, stride=chunks), :]
                    pnow[:, j * 128 : (j + 1) * 128] = value
                    pbf[:, j * 128 : (j + 1) * 128] = value.astype(bf16)
                build_hot()

            def second():
                images.append(row_image_of())
                copies[1].wait()
                copies[2].wait()

            sent = exchange(p, first, second)
            image = images[0]
        else:
            sent = exchange(p, lambda: None, lambda: None)
            wait_stat(it)
            violation = jnp.sum(stat[it], axis=0)[:, 127:128]
            weight = jnp.sqrt(weight * jnp.sqrt((violation + 1e-06) / (change + 1e-06)))
        tau = step_scale / weight
        ends = buf[p, :, SPLIT * main :, :].reshape(n_all * tail, sub)
        moved_sum = jnp.zeros((8, 128), f32)
        for q in range(SPLIT):
            body = buf[p, :, q * main : (q + 1) * main, :].reshape(n_all * main, sub)
            at = n_all * main + q * n_all * tail
            grad = jnp.dot(hot[:, : n_all * main], body, preferred_element_type=f32)
            grad = grad + jnp.dot(
                hot[:, at : at + n_all * tail], ends, preferred_element_type=f32
            )
            for h in range(sub // 128):
                j = q * (sub // 128) + h
                here = pl.ds(j, n_cb, stride=chunks)
                span = slice(j * 128, (j + 1) * 128)
                old = pnow[:, span]
                stepped = old - tau * (cv[here, :] - grad[:, h * 128 : (h + 1) * 128])
                new = jnp.minimum(jnp.maximum(stepped, 0.0), uv[here, :])
                gap = new - old
                moved_sum = moved_sum + jnp.sum((gap * gap).reshape(n_cb // 8, 8, 128), axis=0)
                pnow[:, span] = new
                pbf[:, span] = new.astype(bf16)
                if it == ITERS - 1:
                    pv[here, :] = new
        if it == ITERS - 1:
            leaving = pltpu.make_async_copy(pv, out_primal, local_sem.at[0])
            leaving.start()
        change = jnp.sum(moved_sum, axis=(0, 1), keepdims=True)
        next_image = row_image_of()
        sigma = step_scale * weight
        dual = jnp.maximum(dual + sigma * (bounds - (2.0 * next_image - image)), 0.0)
        short = jnp.maximum(bounds - next_image, 0.0)
        image = next_image
        stat[it + 1, me] = jnp.where(
            lane == 127, jnp.sum(short * short, axis=(0, 1), keepdims=True), 0.0
        )
        for copy in pending:
            copy.wait_send()
        for copy in sent:
            copy.wait_send()
        pending = send_stat(it + 1)

    for e in range(n_dev):
        line = jnp.zeros((1, rows_per), f32)
        for k in range(blocks):
            line = jnp.where(dest[k] == e, dual[k : k + 1, :], line)
        dsend[e] = line
    sent = []
    for k in range(1, n_dev):
        td = (d + k) % n_dev
        copy = remote(dsend.at[td], drecv.at[d], dual_send.at[k], dual_recv.at[d], g, td)
        copy.start()
        sent.append(copy)
    drecv[d] = dsend[d]
    wait_stat(ITERS)
    violation = jnp.sum(stat[ITERS], axis=0)[:, 127:128]
    weight = jnp.sqrt(weight * jnp.sqrt((violation + 1e-06) / (change + 1e-06)))
    out_weight[...] = jnp.broadcast_to(weight, (1, 128))
    for k in range(1, n_dev):
        src = (d + k) % n_dev
        remote(dsend.at[src], drecv.at[src], dual_send.at[k], dual_recv.at[src], g, src).wait_recv()
    out_dual[...] = drecv[...]
    leaving.wait()
    for copy in pending:
        copy.wait_send()
    for copy in sent:
        copy.wait_send()


def fused_device(mesh_shape, *args):
    tiles, cols, counts, dest, row_bounds, dual_start, primal, cost, upper = args
    slots, rows_per, width = tiles.shape
    blocks = counts.shape[0]
    column_blocks = primal.shape[0] // width
    if not fits(mesh_shape, slots, rows_per, width, blocks, column_blocks):
        return per_device(*args)
    n_grp, n_dev = mesh_shape["grp"], mesh_shape["dev"]
    n_all = n_grp * n_dev
    main, tail = tile_split(slots)
    rows_in = (
        jnp.stack([row_bounds, dual_start]).astype(jnp.float32).reshape(2, blocks, rows_per)
    )
    flat = (primal.shape[0] // 128, 128)
    f32, bf16 = jnp.float32, jnp.bfloat16
    vmem = pl.BlockSpec(memory_space=pltpu.VMEM)
    smem = pl.BlockSpec(memory_space=pltpu.SMEM)
    far = pl.BlockSpec(memory_space=pltpu.HBM)
    sends = (n_grp - 1) + n_grp * (n_dev // 2) + n_grp * (n_dev // 2 - 1)
    out_primal, out_dual, out_weight = pl.pallas_call(
        functools.partial(fused_kernel, n_grp, n_dev),
        name="pdhg_fused",
        out_shape=(
            jax.ShapeDtypeStruct(flat, f32),
            jax.ShapeDtypeStruct((n_dev, 1, rows_per), f32),
            jax.ShapeDtypeStruct((1, 128), f32),
        ),
        in_specs=[smem, vmem, far, far, far, far],
        out_specs=(far, vmem, vmem),
        scratch_shapes=[
            pltpu.VMEM((slots, rows_per, width), bf16),
            pltpu.VMEM(flat, f32),
            pltpu.VMEM(flat, f32),
            pltpu.VMEM(flat, f32),
            pltpu.VMEM((column_blocks, width), f32),
            pltpu.VMEM((column_blocks, width), bf16),
            pltpu.VMEM((column_blocks, n_all * (main + SPLIT * tail)), bf16),
            pltpu.VMEM((2, n_all, SPLIT * main + tail, width // SPLIT), bf16),
            pltpu.VMEM((ITERS + 1, n_all, 1, 128), f32),
            pltpu.VMEM((n_dev, 1, rows_per), f32),
            pltpu.VMEM((n_dev, 1, rows_per), f32),
            pltpu.SemaphoreType.DMA((3 + slots // 4,)),
            pltpu.SemaphoreType.DMA((sends,)),
            pltpu.SemaphoreType.DMA((2, n_all)),
            pltpu.SemaphoreType.DMA((ITERS + 1, n_all)),
            pltpu.SemaphoreType.DMA((ITERS + 1, n_all)),
            pltpu.SemaphoreType.DMA((n_dev,)),
            pltpu.SemaphoreType.DMA((n_dev,)),
        ],
        compiler_params=pltpu.CompilerParams(
            collective_id=0, has_side_effects=True, vmem_limit_bytes=65 * 10**6
        ),
    )(
        jnp.concatenate([cols, counts, dest]),
        rows_in,
        tiles,
        primal.reshape(flat),
        cost.reshape(flat),
        upper.reshape(flat),
    )
    return out_primal.reshape(-1), out_dual.reshape(-1), out_weight[0, :1]


def solution(mesh):
    in_specs = (
        P(("grp", "dev"), None, None),
        P(("grp", "dev")),
        P(("grp", "dev")),
        P(("grp", "dev")),
        P(("grp", "dev")),
        P(("grp", "dev")),
        P(),
        P(),
        P(),
    )
    out_specs = (P(), P(("grp", "dev")), P())
    return jax.shard_map(
        functools.partial(fused_device, dict(mesh.shape)),
        mesh=mesh,
        in_specs=in_specs,
        out_specs=out_specs,
        check_vma=False,
    )
```
